128 devices in a mesh: vocab: 8 (over y, z_lo), dp: 16 (over z_hi, x, core).
Axes of the slice: x: 4, y: 4, z: 4 (z_hi: 2, z_lo: 2; z = z_hi * 2 + z_lo), core: 2. Of those that a mesh axis runs over, the one named last changes fastest.
Arguments:
- grads: bfloat16 [16384, 4096], P(('vocab', 'dp')), may hold values from -6 to 6
- token_ids: int32 [16384], P(('vocab', 'dp')), may hold values from 0 to 64127, as said below
Outputs:
- grad_table: float32 [64128, 4096], P('vocab', 'dp')
- row_share: float32 [64128], P('vocab')
The draws below stay inside these ranges and needn't reach their ends.
Inputs may be any that keep to these rules, and one draw needn't show every extreme that they name: `token_ids`: within the 128 ids of one device (aligned blocks in order) the ids never fall; at most 32 of them lie in the rows k * 8016 to (k + 1) * 8016 - 1 of any one k, and in every block some k has exactly 32.
All inputs are finite; a program needn't handle non-finite values.
Results may differ from the reference program's by a relative error of at most 0.0003.
Values may be sent and summed in bfloat16 or wider, within the bound.
A program may use at most 64 MiB of HBM per device.

```python
import jax
import jax.numpy as jnp
from jax import lax

D = 4096
VOCAB_DEV = 8016
TOK_DEV = 128
CAP = 32
VOCAB = 64128
TOKENS = 16384
N_VOCAB = 8


def one_block(key):
    owners = VOCAB // VOCAB_DEV
    base = TOK_DEV // owners
    order = jax.random.permutation(jax.random.fold_in(key, 1), owners)
    top = order[0]
    lowest = order[1]
    counts = jnp.full((owners,), base, jnp.int32)
    counts = counts.at[top].set(CAP).at[lowest].set(2 * base - CAP)
    for turn in range(6):
        sub_key = jax.random.fold_in(key, 10 + turn)
        paired = jax.random.permutation(sub_key, owners)
        first = paired[0]
        second = paired[1]
        keep = jnp.where(second == top, CAP, 0)
        limit = jnp.minimum(CAP - counts[first], counts[second] - keep)
        moved = jax.random.randint(jax.random.fold_in(sub_key, 5), (), 0, limit + 1)
        counts = counts.at[first].add(moved).at[second].add(-moved)
    ends = jnp.cumsum(counts)
    places = jnp.arange(TOK_DEV, dtype=jnp.int32)
    owner_of = jnp.sum((places[:, None] >= ends[None, :]).astype(jnp.int32), axis=1)
    inner = jax.random.randint(jax.random.fold_in(key, 3), (TOK_DEV,), 0, VOCAB_DEV)
    return jnp.sort(owner_of * VOCAB_DEV + inner)


def draw_token_ids(key, part):
    blocks = TOKENS // TOK_DEV
    keys = jax.random.split(jax.random.fold_in(key, 77), blocks)
    return jax.vmap(one_block)(keys).reshape(-1).astype(jnp.int32)


def level_of(own_key, extent, shards, smallest, high):
    def one(axis_at, blocks):
        heights = jax.random.uniform(jax.random.fold_in(jax.random.fold_in(own_key, 6), axis_at), (blocks,), jnp.float32, smallest / len(shards), high / len(shards))
        return jnp.repeat(jnp.exp(heights), extent[axis_at] // blocks).reshape((-1,) + (1,) * (len(extent) - axis_at - 1))

    level = one(*shards[0])
    for cut in shards[1:]:
        level = level * one(*cut)
    return level


def scatter_about(own_key, extent, width, reach, cuts=(), kind=jnp.bfloat16):
    factor_of = level_of(own_key, extent, cuts, -0.22, 0.18) if cuts else 1.0
    drawn = jax.random.normal(own_key, extent, jnp.float32) * width * factor_of
    return jnp.minimum(jnp.maximum(drawn, -reach), reach).astype(kind)


def setup_inputs(seed: int = 0) -> dict:
    splits = jax.random.split(jax.random.key(seed), 3)
    return {
        "grads": scatter_about(splits[0], (TOKENS, D), 1.0, 6.0, ((0, 128),)),
        "token_ids": draw_token_ids(jax.random.fold_in(splits[2], 71), 0),
    }


def reference(grads, token_ids):
    vocab_total = VOCAB_DEV * N_VOCAB
    grad_blocks = grads.reshape(-1, TOK_DEV, D)
    id_blocks = token_ids.reshape(-1, TOK_DEV)

    def accumulate(carry, item):
        table, counts = carry
        block, ids = item
        table = table + jax.ops.segment_sum(block.astype(jnp.float32), ids, num_segments=vocab_total)
        counts = counts + jax.ops.segment_sum(jnp.ones((TOK_DEV,), jnp.float32), ids, num_segments=vocab_total)
        return (table, counts), None

    start = (jnp.zeros((vocab_total, D), jnp.float32), jnp.zeros((vocab_total,), jnp.float32))
    (table, counts), _ = lax.scan(accumulate, start, (grad_blocks, id_blocks))
    row_share = counts * (vocab_total / TOKENS)
    return table, row_share
```

```python
import functools

import jax
import jax.numpy as jnp
from jax import lax
from jax.experimental import pallas as pl
from jax.experimental.pallas import tpu as pltpu
from jax.sharding import PartitionSpec as P

VOCAB_DEV = 8016
TOK_DEV = 128
CAP = 32
COLS = 256
N_V = 8
N_D = 16
N_DEV = N_V * N_D
HI_ROWS = 64
MESH = pl.DeviceIdType.MESH
NT = (((1,), (1,)), ((), ()))

PLANE_A = [(i, 0, 0, j) for j in range(2) for i in range(4)][1:]
PLANE_B = [(0, i, j, 0) for j in range(4) for i in range(4)][1:]


def position():
    v = lax.axis_index("vocab")
    d = lax.axis_index("dp")
    return (d // 2) % 4, v // 2, 2 * (d // 8) + v % 2, d % 2


def device_at(x, y, z, c):
    return y * 2 + z % 2, ((z // 2) * 4 + x) * 2 + c


def offset(k):
    c, a, b, e = k % 2, (k // 2) % 4, (k // 8) % 4, k // 32
    return a, (a + b) % 4, (a + b + e) % 4, c


def exchange(grads_hbm, ids_ref, rows_ref, keys_ref, counts_ref, held, send, id_send, id_recv,
             load_sem, send_sem, recv_sem, id_send_sem, id_recv_sem, own_sem, far_sem):
    x, y, z, c = position()

    def there(o):
        return device_at((x + o[0]) % 4, (y + o[1]) % 4, (z + o[2]) % 4, (c + o[3]) % 2)

    barrier = pltpu.get_barrier_semaphore()
    for o in PLANE_A + PLANE_B:
        pl.semaphore_signal(barrier, inc=1, device_id=there(o), device_id_type=MESH)
    load = pltpu.make_async_copy(grads_hbm, held, load_sem)
    load.start()

    ids = ids_ref[...]
    owner = jnp.zeros_like(ids)
    for v in range(1, N_V):
        owner += (ids >= v * VOCAB_DEV).astype(jnp.int32)
    lane = lax.broadcasted_iota(jnp.int32, (1, TOK_DEV), 1)
    place = lane
    for v in range(1, N_V):
        before = jnp.sum((owner < v).astype(jnp.int32), axis=1, keepdims=True)
        place = place - jnp.where(owner == v, before, 0)
    slot = owner * CAP + place
    select = (lax.broadcasted_iota(jnp.int32, (N_V * CAP, TOK_DEV), 0) == slot).astype(jnp.bfloat16)
    inner = ids - owner * VOCAB_DEV
    mine = lax.broadcasted_iota(jnp.int32, (N_V, TOK_DEV), 0) == owner
    high = jnp.where(mine, inner // 128 + 1, 0).astype(jnp.bfloat16)
    low = jnp.where(mine, inner % 128, 0).astype(jnp.bfloat16)
    spread = (lax.broadcasted_iota(jnp.int32, (TOK_DEV, TOK_DEV), 0) % CAP == place).astype(jnp.bfloat16)
    high_at = lax.dot_general(high, spread, NT, preferred_element_type=jnp.float32)
    low_at = lax.dot_general(low, spread, NT, preferred_element_type=jnp.float32)
    slot_rows = (high_at - 1.0) * 128.0 + low_at
    slot_rows = slot_rows.astype(jnp.int32)
    for v in range(N_V):
        id_send[v] = slot_rows[v : v + 1, :]
    load.wait()
    for d in range(N_D):
        send[d] = jnp.dot(select, held[:, d * COLS : (d + 1) * COLS], preferred_element_type=jnp.float32).astype(jnp.bfloat16)

    pl.semaphore_wait(barrier, len(PLANE_A) + len(PLANE_B))
    for o in PLANE_B:
        pl.semaphore_signal(far_sem, inc=1, device_id=there(o), device_id_type=MESH)
    pl.semaphore_wait(far_sem, len(PLANE_B))

    @pl.loop(1, N_DEV)
    def _(k):
        v, d = there(offset(k))
        pltpu.make_async_remote_copy(
            id_send.at[v], id_recv.at[(k % 4) * CAP + k // 4], id_send_sem, id_recv_sem, device_id=(v, d), device_id_type=MESH
        ).start()
        pltpu.make_async_remote_copy(
            send.at[d, pl.ds(pl.multiple_of(v * CAP, CAP), CAP)], rows_ref.at[k], send_sem, recv_sem.at[k // 16],
            device_id=(v, d), device_id_type=MESH
        ).start()

    v, d = device_at(x, y, z, c)
    own = pltpu.make_async_copy(send.at[d, pl.ds(pl.multiple_of(v * CAP, CAP), CAP)], rows_ref.at[0], own_sem)
    own.start()
    id_recv[0] = id_send[v]

    id_got = id_recv.at[pl.ds(1, N_DEV - 1)]
    pltpu.make_async_copy(id_got, id_got, id_recv_sem).wait()
    group = lax.broadcasted_iota(jnp.int32, (CAP, 128), 1) // CAP
    keys = jnp.zeros((CAP, 128), jnp.int32)
    for i in range(4):
        keys = jnp.where(group == i, id_recv[i * CAP : (i + 1) * CAP, 0, :], keys)
    keys_ref[...] = keys

    tall = lax.broadcasted_iota(jnp.int32, (128, 128), 0)
    total = jnp.zeros((HI_ROWS, 128), jnp.float32)
    for q in range(CAP):
        row = keys_ref[q : q + 1, :]
        hot_high = (tall[:HI_ROWS] == row // 128).astype(jnp.bfloat16)
        hot_low = (tall == row % 128).astype(jnp.bfloat16)
        total = total + lax.dot_general(hot_high, hot_low, NT, preferred_element_type=jnp.float32)
    counts_ref[...] = total * (VOCAB_DEV / (TOK_DEV * N_D))

    own.wait()
    first = rows_ref.at[pl.ds(1, 15)]
    pltpu.make_async_copy(first, first, recv_sem.at[0]).wait()
    for g in range(1, 8):
        got = rows_ref.at[pl.ds(16 * g, 16)]
        pltpu.make_async_copy(got, got, recv_sem.at[g]).wait()
    sent = rows_ref.at[pl.ds(1, N_DEV - 1)]
    pltpu.make_async_copy(sent, sent, send_sem).wait()
    pltpu.make_async_copy(id_got, id_got, id_send_sem).wait()


TILE = 512


def scatter(rows_ref, keys_ref, table_ref):
    first = pl.program_id(0) * TILE
    at = lax.broadcasted_iota(jnp.int32, (TILE, 128), 0) + first
    total = jnp.zeros((TILE, COLS), jnp.float32)
    for g in range(8):
        hots = [(at == keys_ref[4 * g + i : 4 * g + i + 1, :]).astype(jnp.bfloat16) for i in range(4)]
        total = total + jnp.dot(
            jnp.concatenate(hots, axis=1), rows_ref[512 * g : 512 * (g + 1), :], preferred_element_type=jnp.float32
        )
    table_ref[...] = total


def local(grads, token_ids):
    vmem = pl.BlockSpec(memory_space=pltpu.VMEM)
    dma = pltpu.SemaphoreType.DMA
    rows, keys, counts = pl.pallas_call(
        exchange,
        out_shape=(
            jax.ShapeDtypeStruct((N_DEV, CAP, COLS), jnp.bfloat16),
            jax.ShapeDtypeStruct((CAP, 128), jnp.int32),
            jax.ShapeDtypeStruct((HI_ROWS, 128), jnp.float32),
        ),
        in_specs=[pl.BlockSpec(memory_space=pl.ANY), vmem],
        out_specs=(vmem, vmem, vmem),
        scratch_shapes=[
            pltpu.VMEM((TOK_DEV, N_D * COLS), jnp.bfloat16),
            pltpu.VMEM((N_D, N_V * CAP, COLS), jnp.bfloat16),
            pltpu.VMEM((N_V, 1, 128), jnp.int32),
            pltpu.VMEM((N_DEV, 1, 128), jnp.int32),
            dma, dma, dma((8,)), dma, dma, dma, pltpu.SemaphoreType.REGULAR,
        ],
        compiler_params=pltpu.CompilerParams(collective_id=0, has_side_effects=True),
        name="exchange",
    )(grads, token_ids.reshape(1, TOK_DEV))
    table = pl.pallas_call(
        scatter,
        out_shape=jax.ShapeDtypeStruct((VOCAB_DEV, COLS), jnp.float32),
        grid=(pl.cdiv(VOCAB_DEV, TILE),),
        in_specs=[
            pl.BlockSpec((N_DEV * CAP, COLS), lambda i: (0, 0)),
            pl.BlockSpec((CAP, 128), lambda i: (0, 0)),
        ],
        out_specs=pl.BlockSpec((TILE, COLS), lambda i: (i, 0)),
        name="scatter",
    )(rows.reshape(N_DEV * CAP, COLS), keys)
    return table, counts.reshape(-1)[:VOCAB_DEV]


def solution(mesh):
    in_specs = (P(("vocab", "dp"), None), P(("vocab", "dp")))
    out_specs = (P("vocab", "dp"), P("vocab"))
    return jax.shard_map(local, mesh=mesh, in_specs=in_specs, out_specs=out_specs, check_vma=False)
```

```python
import functools

import jax
import jax.numpy as jnp
from jax import lax
from jax.experimental import pallas as pl
from jax.experimental.pallas import tpu as pltpu
from jax.sharding import PartitionSpec as P

VOCAB_DEV = 8016
TOK_DEV = 128
CAP = 32
COLS = 256
N_V = 8
N_D = 16
N_DEV = N_V * N_D
HI_ROWS = 64
PAD_ROWS = 8064
STRIPE = 4032
TILE = 1344
GROUPS = 8
MESH = pl.DeviceIdType.MESH
NT = (((1,), (1,)), ((), ()))

PLANE_A = [(i, 0, 0, j) for j in range(2) for i in range(4)][1:]
PLANE_B = [(0, i, j, 0) for j in range(4) for i in range(4)][1:]


def position():
    v = lax.axis_index("vocab")
    d = lax.axis_index("dp")
    return (d // 2) % 4, v // 2, 2 * (d // 8) + v % 2, d % 2


def device_at(x, y, z, c):
    return y * 2 + z % 2, ((z // 2) * 4 + x) * 2 + c


def offset(k):
    c, a, b, e = k % 2, (k // 2) % 4, (k // 8) % 4, k // 32
    return a, (a + b) % 4, (a + b + e) % 4, c


def exchange(grads_hbm, ids_ref, table_ref, last_ref, keys_ref, counts_ref, held, send, id_send, id_recv, rows_ref,
             load_sem, send_sem, recv_sem, id_send_sem, id_recv_sem, own_sem, far_sem):
    x, y, z, c = position()

    def there(o):
        return device_at((x + o[0]) % 4, (y + o[1]) % 4, (z + o[2]) % 4, (c + o[3]) % 2)

    barrier = pltpu.get_barrier_semaphore()
    for o in PLANE_A + PLANE_B:
        pl.semaphore_signal(barrier, inc=1, device_id=there(o), device_id_type=MESH)
    load = pltpu.make_async_copy(grads_hbm, held, load_sem)
    load.start()

    ids = ids_ref[...]
    owner = jnp.zeros_like(ids)
    for v in range(1, N_V):
        owner += (ids >= v * VOCAB_DEV).astype(jnp.int32)
    lane = lax.broadcasted_iota(jnp.int32, (1, TOK_DEV), 1)
    place = lane
    for v in range(1, N_V):
        before = jnp.sum((owner < v).astype(jnp.int32), axis=1, keepdims=True)
        place = place - jnp.where(owner == v, before, 0)
    slot = owner * CAP + place
    select = (lax.broadcasted_iota(jnp.int32, (N_V * CAP, TOK_DEV), 0) == slot).astype(jnp.bfloat16)
    inner = ids - owner * VOCAB_DEV
    mine = lax.broadcasted_iota(jnp.int32, (N_V, TOK_DEV), 0) == owner
    high = jnp.where(mine, inner // 128 + 1, 0).astype(jnp.bfloat16)
    low = jnp.where(mine, inner % 128, 0).astype(jnp.bfloat16)
    spread = (lax.broadcasted_iota(jnp.int32, (TOK_DEV, TOK_DEV), 0) % CAP == place).astype(jnp.bfloat16)
    high_at = lax.dot_general(high, spread, NT, preferred_element_type=jnp.float32)
    low_at = lax.dot_general(low, spread, NT, preferred_element_type=jnp.float32)
    slot_rows = (high_at - 1.0) * 128.0 + low_at
    slot_rows = slot_rows.astype(jnp.int32)
    for v in range(N_V):
        id_send[v] = slot_rows[v : v + 1, :]
    load.wait()
    for d in range(N_D):
        send[d] = jnp.dot(select, held[:, d * COLS : (d + 1) * COLS], preferred_element_type=jnp.float32).astype(jnp.bfloat16)

    pl.semaphore_wait(barrier, len(PLANE_A) + len(PLANE_B))
    for o in PLANE_B:
        pl.semaphore_signal(far_sem, inc=1, device_id=there(o), device_id_type=MESH)
    pl.semaphore_wait(far_sem, len(PLANE_B))

    @pl.loop(1, N_DEV)
    def _(k):
        v, d = there(offset(k))
        pltpu.make_async_remote_copy(
            id_send.at[v], id_recv.at[(k % 4) * CAP + k // 4], id_send_sem, id_recv_sem, device_id=(v, d), device_id_type=MESH
        ).start()
        pltpu.make_async_remote_copy(
            send.at[d, pl.ds(pl.multiple_of(v * CAP, CAP), CAP)], rows_ref.at[k], send_sem, recv_sem.at[k // 16],
            device_id=(v, d), device_id_type=MESH
        ).start()

    v, d = device_at(x, y, z, c)
    own = pltpu.make_async_copy(send.at[d, pl.ds(pl.multiple_of(v * CAP, CAP), CAP)], rows_ref.at[0], own_sem)
    own.start()
    id_recv[0] = id_send[v]

    id_got = id_recv.at[pl.ds(1, N_DEV - 1)]
    pltpu.make_async_copy(id_got, id_got, id_recv_sem).wait()
    group = lax.broadcasted_iota(jnp.int32, (CAP, 128), 1) // CAP
    keys = jnp.zeros((CAP, 128), jnp.int32)
    for i in range(4):
        keys = jnp.where(group == i, id_recv[i * CAP : (i + 1) * CAP, 0, :], keys)
    keys_ref[...] = keys

    tall = lax.broadcasted_iota(jnp.int32, (128, 128), 0)
    total = jnp.zeros((HI_ROWS, 128), jnp.float32)
    for q in range(CAP):
        row = keys_ref[q : q + 1, :]
        hot_high = (tall[:HI_ROWS] == row // 128).astype(jnp.bfloat16)
        hot_low = (tall == row % 128).astype(jnp.bfloat16)
        total = total + lax.dot_general(hot_high, hot_low, NT, preferred_element_type=jnp.float32)
    counts_ref[...] = total * (VOCAB_DEV / (TOK_DEV * N_D))

    def add_group(g, start):
        rows = rows_ref[pl.ds(pl.multiple_of(16 * g, 16), 16)].reshape(16 * CAP, COLS)
        keys = [keys_ref[pl.ds(4 * g + i, 1), :] for i in range(4)]

        @pl.loop(0, PAD_ROWS // STRIPE)
        def _(t):
            at = lax.broadcasted_iota(jnp.int32, (STRIPE, 128), 0) + t * STRIPE
            hot = jnp.concatenate([(at == key).astype(jnp.bfloat16) for key in keys], axis=1)
            part = jnp.dot(hot, rows, preferred_element_type=jnp.float32)
            here = pl.ds(pl.multiple_of(t * STRIPE, STRIPE), STRIPE)
            if start:
                table_ref[here, :] = part
            else:
                table_ref[here, :] += part

    own.wait()
    first = rows_ref.at[pl.ds(1, 15)]
    pltpu.make_async_copy(first, first, recv_sem.at[0]).wait()
    add_group(0, True)

    @pl.loop(1, GROUPS - 1)
    def _(g):
        got = rows_ref.at[pl.ds(pl.multiple_of(16 * g, 16), 16)]
        pltpu.make_async_copy(got, got, recv_sem.at[g]).wait()
        add_group(g, False)

    got = rows_ref.at[pl.ds(16 * (GROUPS - 1), 16)]
    pltpu.make_async_copy(got, got, recv_sem.at[GROUPS - 1]).wait()
    last_ref[...] = rows_ref[16 * (GROUPS - 1) :].reshape(last_ref.shape)
    sent = rows_ref.at[pl.ds(1, N_DEV - 1)]
    pltpu.make_async_copy(sent, sent, send_sem).wait()
    pltpu.make_async_copy(id_got, id_got, id_send_sem).wait()


def finish(table_ref, last_ref, keys_ref, out_ref):
    first = pl.program_id(0) * TILE
    at = lax.broadcasted_iota(jnp.int32, (TILE, 128), 0) + first
    hot = jnp.concatenate([(at == keys_ref[4 * (GROUPS - 1) + i : 4 * (GROUPS - 1) + i + 1, :]).astype(jnp.bfloat16) for i in range(4)], axis=1)
    out_ref[...] = table_ref[pl.ds(pl.multiple_of(first, TILE), TILE), :] + jnp.dot(hot, last_ref[...], preferred_element_type=jnp.float32)


def local(grads, token_ids):
    vmem = pl.BlockSpec(memory_space=pltpu.VMEM)
    dma = pltpu.SemaphoreType.DMA
    table, last, keys, counts = pl.pallas_call(
        exchange,
        out_shape=(
            pltpu.VMEM((PAD_ROWS, COLS), jnp.float32),
            pltpu.VMEM((16 * CAP, COLS), jnp.bfloat16),
            pltpu.VMEM((CAP, 128), jnp.int32),
            jax.ShapeDtypeStruct((HI_ROWS, 128), jnp.float32),
        ),
        in_specs=[pl.BlockSpec(memory_space=pltpu.HBM), vmem],
        out_specs=(vmem, vmem, vmem, vmem),
        scratch_shapes=[
            pltpu.VMEM((TOK_DEV, N_D * COLS), jnp.bfloat16),
            pltpu.VMEM((N_D, N_V * CAP, COLS), jnp.bfloat16),
            pltpu.VMEM((N_V, 1, 128), jnp.int32),
            pltpu.VMEM((N_DEV, 1, 128), jnp.int32),
            pltpu.VMEM((N_DEV, CAP, COLS), jnp.bfloat16),
            dma, dma, dma((8,)), dma, dma, dma, pltpu.SemaphoreType.REGULAR,
        ],
        compiler_params=pltpu.CompilerParams(collective_id=0, has_side_effects=True, vmem_limit_bytes=36 << 20),
        name="exchange",
    )(grads, token_ids.reshape(1, TOK_DEV))
    out = pl.pallas_call(
        finish,
        out_shape=jax.ShapeDtypeStruct((VOCAB_DEV, COLS), jnp.float32),
        grid=(PAD_ROWS // TILE,),
        in_specs=[vmem, vmem, vmem],
        out_specs=pl.BlockSpec((TILE, COLS), lambda i: (i, 0)),
        compiler_params=pltpu.CompilerParams(vmem_limit_bytes=24 << 20),
        name="finish",
    )(table, last, keys)
    return out, counts.reshape(-1)[:VOCAB_DEV]


def solution(mesh):
    in_specs = (P(("vocab", "dp"), None), P(("vocab", "dp")))
    out_specs = (P("vocab", "dp"), P("vocab"))
    return jax.shard_map(local, mesh=mesh, in_specs=in_specs, out_specs=out_specs, check_vma=False)
```

```python
import jax
import jax.numpy as jnp
from jax import lax
from jax.experimental import pallas as pl
from jax.experimental.pallas import tpu as pltpu
from jax.sharding import PartitionSpec as P

VOCAB_DEV = 8016
TOK_DEV = 128
CAP = 32
COLS = 256
N_V = 8
N_D = 16
N_DEV = N_V * N_D
HI_ROWS = 64
PAD_ROWS = 8064
STRIPE = 4032
PIECES = (1344,) * 5 + (1296,)
MESH = pl.DeviceIdType.MESH
NT = (((1,), (1,)), ((), ()))

PLANE_A = [(i, 0, 0, j) for i in range(4) for j in range(2)]
PLANE_B = [(0, i, j, 0) for i in range(4) for j in range(4)]
NEAR = PLANE_A + PLANE_B[1:]
FAR = [
    (k // 2 % 4, (k // 2 + k // 8) % 4, (k // 2 + k // 8 + k // 32) % 4, k % 2)
    for k in range(N_DEV)
]
ORDER = NEAR + [o for o in FAR if o not in NEAR]
GROUPS = [(0, 16), (16, 16), (32, 16), (48, 16), (64, 16), (80, 16), (96, 16), (112, 8), (120, 8)]
LAST = GROUPS[-1][0]


def exchange(grads_hbm, ids_hbm, table_ref, last_ref, keys_ref, share_ref, held, ids_ref, send, ids_a, ids_b, rows_ref,
             load_sem, id_load_sem, send_sem, recv_sem, a_send_sem, a_recv_sem, b_send_sem, b_recv_sem, own_sem):
    v = lax.axis_index("vocab")
    d = lax.axis_index("dp")
    y, zl, zh, x, c = v // 2, v % 2, d // 8, (d // 2) % 4, d % 2
    z = 2 * zh + zl
    at_x = [2 * lax.rem(x + i, 4) for i in range(4)]
    at_y = [2 * lax.rem(y + i, 4) for i in range(4)]
    at_z = [lax.rem(z + i, 4) for i in range(4)]
    at_c = [c, 1 - c]
    vocab_at = [[at_y[i] + lax.rem(at_z[j], 2) for j in range(4)] for i in range(4)]
    data_at = [[at_x[i] + at_c[j] for j in range(2)] for i in range(4)]
    high_at = [8 * (at_z[j] // 2) for j in range(4)]

    def there(o):
        return vocab_at[o[1]][o[2]], data_at[o[0]][o[3]] + high_at[o[2]]

    barrier = pltpu.get_barrier_semaphore()
    for o in NEAR[1:]:
        pl.semaphore_signal(barrier, inc=1, device_id=there(o), device_id_type=MESH)
    id_load = pltpu.make_async_copy(ids_hbm, ids_ref, id_load_sem)
    id_load.start()
    load = pltpu.make_async_copy(grads_hbm, held, load_sem)
    load.start()

    id_load.wait()
    ids = ids_ref[...]
    owner = jnp.zeros_like(ids)
    for i in range(1, N_V):
        owner += (ids >= i * VOCAB_DEV).astype(jnp.int32)
    place = lax.broadcasted_iota(jnp.int32, (1, TOK_DEV), 1)
    for i in range(1, N_V):
        before = jnp.sum((owner < i).astype(jnp.int32), axis=1, keepdims=True)
        place = place - jnp.where(owner == i, before, 0)
    select = (lax.broadcasted_iota(jnp.int32, (N_V * CAP, TOK_DEV), 0) == owner * CAP + place).astype(jnp.bfloat16)
    inner = ids - owner * VOCAB_DEV
    mine = lax.broadcasted_iota(jnp.int32, (N_V, TOK_DEV), 0) == owner
    high = jnp.where(mine, inner // 128 + 1, 0).astype(jnp.bfloat16)
    low = jnp.where(mine, inner % 128, 0).astype(jnp.bfloat16)
    spread = (lax.broadcasted_iota(jnp.int32, (TOK_DEV, TOK_DEV), 0) % CAP == place).astype(jnp.bfloat16)
    high_of = lax.dot_general(high, spread, NT, preferred_element_type=jnp.float32)
    low_of = lax.dot_general(low, spread, NT, preferred_element_type=jnp.float32)
    slot_rows = ((high_of - 1.0) * 128.0 + low_of).astype(jnp.int32)
    for i in range(N_V):
        ids_a[0, i] = slot_rows[i : i + 1, :]
    load.wait()
    for i in range(N_D):
        send[i] = jnp.dot(select, held[:, i * COLS : (i + 1) * COLS], preferred_element_type=jnp.float32).astype(jnp.bfloat16)

    def post(k):
        to_v, to_d = there(ORDER[k])
        group = next(g for g, (first, n) in enumerate(GROUPS) if first <= k < first + n)
        pltpu.make_async_remote_copy(
            send.at[to_d, pl.ds(pl.multiple_of(to_v * CAP, CAP), CAP)],
            last_ref.at[k - LAST] if k >= LAST else rows_ref.at[k],
            send_sem, recv_sem.at[group], device_id=(to_v, to_d), device_id_type=MESH,
        ).start()

    pl.semaphore_wait(barrier, len(NEAR) - 1)
    for i, o in enumerate(PLANE_A):
        if i:
            pltpu.make_async_remote_copy(
                ids_a.at[0], ids_a.at[i], a_send_sem, a_recv_sem, device_id=there(o), device_id_type=MESH
            ).start()
    for k in range(1, 8):
        post(k)
    own = pltpu.make_async_copy(send.at[d, pl.ds(pl.multiple_of(v * CAP, CAP), CAP)], rows_ref.at[0], own_sem)
    own.start()
    got_a = ids_a.at[pl.ds(1, 7)]
    pltpu.make_async_copy(got_a, got_a, a_recv_sem).wait()
    for i, o in enumerate(PLANE_B):
        if i:
            to_v, to_d = there(o)
            pltpu.make_async_remote_copy(
                ids_a.at[:, to_v], ids_b.at[i], b_send_sem, b_recv_sem, device_id=(to_v, to_d), device_id_type=MESH
            ).start()
    for k in range(8, len(NEAR)):
        post(k)
    ids_b[0] = ids_a[:, v]
    got_b = ids_b.at[pl.ds(1, 15)]
    pltpu.make_async_copy(got_b, got_b, b_recv_sem).wait()
    for k in range(len(NEAR), N_DEV):
        post(k)

    quarter = lax.broadcasted_iota(jnp.int32, (1, 128), 1) // CAP
    for q in range(CAP):
        key = jnp.zeros((1, 128), jnp.int32)
        for i in range(4):
            o = ORDER[4 * q + i]
            from_b = ids_b[PLANE_B.index((0, o[1], o[2], 0)), PLANE_A.index((o[0], 0, 0, o[3]))]
            key = jnp.where(quarter == i, from_b, key)
        keys_ref[q : q + 1, :] = key

    tall = lax.broadcasted_iota(jnp.int32, (128, 128), 0)
    total = jnp.zeros((HI_ROWS, 128), jnp.float32)
    for q in range(CAP):
        row = keys_ref[q : q + 1, :]
        hot_high = (tall[:HI_ROWS] == row // 128).astype(jnp.bfloat16)
        hot_low = (tall == row % 128).astype(jnp.bfloat16)
        total = total + lax.dot_general(hot_high, hot_low, NT, preferred_element_type=jnp.float32)
    share_ref[...] = total * (VOCAB_DEV / (TOK_DEV * N_D))

    def add(first, n, start=False):
        rows = rows_ref[pl.ds(first, n)].reshape(n * CAP, COLS)
        keys = [keys_ref[pl.ds(first // 4 + i, 1), :] for i in range(n // 4)]

        @pl.loop(0, PAD_ROWS // STRIPE)
        def _(t):
            at = lax.broadcasted_iota(jnp.int32, (STRIPE, 128), 0) + t * STRIPE
            hot = jnp.concatenate([(at == key).astype(jnp.bfloat16) for key in keys], axis=1)
            part = jnp.dot(hot, rows, preferred_element_type=jnp.float32)
            here = pl.ds(pl.multiple_of(t * STRIPE, STRIPE), STRIPE)
            if start:
                table_ref[here, :] = part
            else:
                table_ref[here, :] += part

    def arrived(first, n, group):
        got = rows_ref.at[pl.ds(first, n)]
        pltpu.make_async_copy(got, got, recv_sem.at[group]).wait()

    own.wait()
    arrived(1, 15, 0)
    add(0, 16, True)

    @pl.loop(1, 7)
    def _(g):
        first = pl.multiple_of(16 * g, 16)
        arrived(first, 16, g)
        add(first, 16)

    arrived(112, 8, 7)
    add(112, 8)
    pltpu.make_async_copy(last_ref, last_ref, recv_sem.at[8]).wait()
    sent = rows_ref.at[pl.ds(1, N_DEV - 1)]
    pltpu.make_async_copy(sent, sent, send_sem).wait()
    pltpu.make_async_copy(got_a, got_a, a_send_sem).wait()
    pltpu.make_async_copy(got_b, got_b, b_send_sem).wait()


def finish(table_ref, last_ref, keys_ref, share_ref, table_hbm, share_hbm, stage, sems):
    share = pltpu.make_async_copy(share_ref, share_hbm, sems.at[len(PIECES)])
    share.start()
    n = GROUPS[-1][1]
    rows = last_ref[...].reshape(n * CAP, COLS)
    first = 0
    copies = [share]
    for i, size in enumerate(PIECES):
        at = lax.broadcasted_iota(jnp.int32, (size, 128), 0) + first
        keys = [keys_ref[LAST // 4 + j : LAST // 4 + j + 1, :] for j in range(n // 4)]
        hot = jnp.concatenate([(at == key).astype(jnp.bfloat16) for key in keys], axis=1)
        here = pl.ds(first, size)
        stage[here, :] = table_ref[here, :] + jnp.dot(hot, rows, preferred_element_type=jnp.float32)
        copy = pltpu.make_async_copy(stage.at[here], table_hbm.at[here], sems.at[i])
        copy.start()
        copies.append(copy)
        first += size
    for copy in copies:
        copy.wait()


def local(grads, token_ids):
    vmem = pl.BlockSpec(memory_space=pltpu.VMEM)
    hbm = pl.BlockSpec(memory_space=pltpu.HBM)
    dma = pltpu.SemaphoreType.DMA
    table, last, keys, share = pl.pallas_call(
        exchange,
        out_shape=(
            pltpu.VMEM((PAD_ROWS, COLS), jnp.float32),
            pltpu.VMEM((GROUPS[-1][1], CAP, COLS), jnp.bfloat16),
            pltpu.VMEM((CAP, 128), jnp.int32),
            pltpu.VMEM((HI_ROWS, 128), jnp.float32),
        ),
        in_specs=[hbm, hbm],
        out_specs=(vmem, vmem, vmem, vmem),
        scratch_shapes=[
            pltpu.VMEM((TOK_DEV, N_D * COLS), jnp.bfloat16),
            pltpu.VMEM((1, TOK_DEV), jnp.int32),
            pltpu.VMEM((N_D, N_V * CAP, COLS), jnp.bfloat16),
            pltpu.VMEM((8, N_V, 1, 128), jnp.int32),
            pltpu.VMEM((16, 8, 1, 128), jnp.int32),
            pltpu.VMEM((N_DEV, CAP, COLS), jnp.bfloat16),
            dma, dma, dma, dma((len(GROUPS),)), dma, dma, dma, dma, dma,
        ],
        compiler_params=pltpu.CompilerParams(collective_id=0, has_side_effects=True, vmem_limit_bytes=36 << 20),
        name="exchange",
    )(
        pltpu.with_memory_space_constraint(grads, pltpu.HBM),
        pltpu.with_memory_space_constraint(token_ids.reshape(1, TOK_DEV), pltpu.HBM),
    )
    table, share = pl.pallas_call(
        finish,
        out_shape=(
            jax.ShapeDtypeStruct((VOCAB_DEV, COLS), jnp.float32),
            jax.ShapeDtypeStruct((HI_ROWS, 128), jnp.float32),
        ),
        in_specs=[vmem, vmem, vmem, vmem],
        out_specs=(hbm, hbm),
        scratch_shapes=[pltpu.VMEM((VOCAB_DEV, COLS), jnp.float32), dma((len(PIECES) + 1,))],
        compiler_params=pltpu.CompilerParams(vmem_limit_bytes=32 << 20),
        name="finish",
    )(table, last, keys, share)
    return table, share.reshape(-1)[:VOCAB_DEV]


def solution(mesh):
    in_specs = (P(("vocab", "dp"), None), P(("vocab", "dp")))
    out_specs = (P("vocab", "dp"), P("vocab"))
    return jax.shard_map(local, mesh=mesh, in_specs=in_specs, out_specs=out_specs, check_vma=False)
```

```python
import jax
import jax.numpy as jnp
from jax import lax
from jax.experimental import pallas as pl
from jax.experimental.pallas import tpu as pltpu
from jax.sharding import PartitionSpec as P

VOCAB_DEV = 8016
TOK_DEV = 128
CAP = 32
COLS = 256
N_V = 8
N_D = 16
N_DEV = N_V * N_D
HI_ROWS = 64
PAD_ROWS = 8064
STRIPE = 4032
PIECES = (1344,) * 5 + (1296,)
MESH = pl.DeviceIdType.MESH
NT = (((1,), (1,)), ((), ()))

PLANE_A = [(i, 0, 0, j) for i in range(4) for j in range(2)]
PLANE_B = [(0, i, j, 0) for i in range(4) for j in range(4)]
NEAR = PLANE_A + PLANE_B[1:]
FAR = [
    (k // 2 % 4, (k // 2 + k // 8) % 4, (k // 2 + k // 8 + k // 32) % 4, k % 2)
    for k in range(N_DEV)
]
ORDER = NEAR + [o for o in FAR if o not in NEAR]
GROUPS = [(0, 16), (16, 16), (32, 16), (48, 16), (64, 16), (80, 16), (96, 16), (112, 16)]
AHEAD = 3
LAST = GROUPS[-1][0]


def exchange(grads_hbm, ids_hbm, table_ref, last_ref, keys_ref, share_ref, held, ids_ref, send, id_send, id_recv, rows_ref,
             load_sem, id_load_sem, send_sem, recv_sem, id_send_sem, id_recv_sem, own_sem, far_sem):
    v = lax.axis_index("vocab")
    d = lax.axis_index("dp")
    y, zl, zh, x, c = v // 2, v % 2, d // 8, (d // 2) % 4, d % 2
    z = 2 * zh + zl
    at_x = [2 * lax.rem(x + i, 4) for i in range(4)]
    at_y = [2 * lax.rem(y + i, 4) for i in range(4)]
    at_z = [lax.rem(z + i, 4) for i in range(4)]
    at_c = [c, 1 - c]
    vocab_at = [[at_y[i] + lax.rem(at_z[j], 2) for j in range(4)] for i in range(4)]
    data_at = [[at_x[i] + at_c[j] for j in range(2)] for i in range(4)]
    high_at = [8 * (at_z[j] // 2) for j in range(4)]

    def there(o):
        return vocab_at[o[1]][o[2]], data_at[o[0]][o[3]] + high_at[o[2]]

    barrier = pltpu.get_barrier_semaphore()
    for o in NEAR[1:]:
        pl.semaphore_signal(barrier, inc=1, device_id=there(o), device_id_type=MESH)
    id_load = pltpu.make_async_copy(ids_hbm, ids_ref, id_load_sem)
    id_load.start()
    load = pltpu.make_async_copy(grads_hbm, held, load_sem)
    load.start()

    id_load.wait()
    ids = ids_ref[...]
    owner = jnp.zeros_like(ids)
    for i in range(1, N_V):
        owner += (ids >= i * VOCAB_DEV).astype(jnp.int32)
    place = lax.broadcasted_iota(jnp.int32, (1, TOK_DEV), 1)
    for i in range(1, N_V):
        before = jnp.sum((owner < i).astype(jnp.int32), axis=1, keepdims=True)
        place = place - jnp.where(owner == i, before, 0)
    select = (lax.broadcasted_iota(jnp.int32, (N_V * CAP, TOK_DEV), 0) == owner * CAP + place).astype(jnp.bfloat16)
    inner = ids - owner * VOCAB_DEV
    mine = lax.broadcasted_iota(jnp.int32, (N_V, TOK_DEV), 0) == owner
    high = jnp.where(mine, inner // 128 + 1, 0).astype(jnp.bfloat16)
    low = jnp.where(mine, inner % 128, 0).astype(jnp.bfloat16)
    spread = (lax.broadcasted_iota(jnp.int32, (TOK_DEV, TOK_DEV), 0) % CAP == place).astype(jnp.bfloat16)
    high_of = lax.dot_general(high, spread, NT, preferred_element_type=jnp.float32)
    low_of = lax.dot_general(low, spread, NT, preferred_element_type=jnp.float32)
    slot_rows = ((high_of - 1.0) * 128.0 + low_of).astype(jnp.int32)
    for i in range(N_V):
        id_send[i] = slot_rows[i : i + 1, :]
    load.wait()
    for i in range(N_D):
        send[i] = jnp.dot(select, held[:, i * COLS : (i + 1) * COLS], preferred_element_type=jnp.float32).astype(jnp.bfloat16)

    def post(k):
        to_v, to_d = there(ORDER[k])
        group = next(g for g, (first, n) in enumerate(GROUPS) if first <= k < first + n)
        pltpu.make_async_remote_copy(
            id_send.at[to_v], id_recv.at[k], id_send_sem, id_recv_sem.at[group], device_id=(to_v, to_d), device_id_type=MESH
        ).start()
        pltpu.make_async_remote_copy(
            send.at[to_d, pl.ds(pl.multiple_of(to_v * CAP, CAP), CAP)],
            last_ref.at[k - LAST] if k >= LAST else rows_ref.at[k],
            send_sem, recv_sem.at[group], device_id=(to_v, to_d), device_id_type=MESH,
        ).start()

    pl.semaphore_wait(barrier, len(NEAR) - 1)
    for o in PLANE_B[1:]:
        pl.semaphore_signal(far_sem, inc=1, device_id=there(o), device_id_type=MESH)
    for k in range(1, len(NEAR)):
        post(k)
    own = pltpu.make_async_copy(send.at[d, pl.ds(pl.multiple_of(v * CAP, CAP), CAP)], rows_ref.at[0], own_sem)
    own.start()
    id_recv[0] = id_send[v]
    pl.semaphore_wait(far_sem, len(PLANE_B) - 1)
    for k in range(len(NEAR), sum(GROUPS[AHEAD - 1])):
        post(k)

    def post_after(g):
        if g + AHEAD < len(GROUPS):
            first, n = GROUPS[g + AHEAD]
            for k in range(first, first + n):
                post(k)

    quarter = lax.broadcasted_iota(jnp.int32, (1, 128), 1) // CAP
    tall = lax.broadcasted_iota(jnp.int32, (128, 128), 0)

    def learn(g):
        first, n = GROUPS[g]
        skip = int(g == 0)
        got = id_recv.at[pl.ds(first + skip, n - skip)]
        pltpu.make_async_copy(got, got, id_recv_sem.at[g]).wait()
        hot_high, hot_low = [], []
        for q in range(first // 4, (first + n) // 4):
            key = id_recv[4 * q]
            for i in range(1, 4):
                key = jnp.where(quarter == i, id_recv[4 * q + i], key)
            keys_ref[q : q + 1, :] = key
            hot_high.append((tall[:HI_ROWS] == key // 128).astype(jnp.bfloat16))
            hot_low.append((tall == key % 128).astype(jnp.bfloat16))
        found = lax.dot_general(
            jnp.concatenate(hot_high, axis=1), jnp.concatenate(hot_low, axis=1), NT, preferred_element_type=jnp.float32
        ) * (VOCAB_DEV / (TOK_DEV * N_D))
        if g == 0:
            share_ref[...] = found
        else:
            share_ref[...] += found

    def add(first, n, start=False):
        rows = rows_ref[pl.ds(first, n)].reshape(n * CAP, COLS)
        keys = [keys_ref[pl.ds(first // 4 + i, 1), :] for i in range(n // 4)]

        @pl.loop(0, PAD_ROWS // STRIPE)
        def _(t):
            at = lax.broadcasted_iota(jnp.int32, (STRIPE, 128), 0) + t * STRIPE
            hot = jnp.concatenate([(at == key).astype(jnp.bfloat16) for key in keys], axis=1)
            part = jnp.dot(hot, rows, preferred_element_type=jnp.float32)
            here = pl.ds(pl.multiple_of(t * STRIPE, STRIPE), STRIPE)
            if start:
                table_ref[here, :] = part
            else:
                table_ref[here, :] += part

    def arrived(first, n, group):
        got = rows_ref.at[pl.ds(first, n)]
        pltpu.make_async_copy(got, got, recv_sem.at[group]).wait()

    learn(0)
    own.wait()
    arrived(1, GROUPS[0][1] - 1, 0)
    post_after(0)
    add(0, GROUPS[0][1], True)
    for g in range(1, len(GROUPS) - 1):
        learn(g)
        arrived(*GROUPS[g], g)
        post_after(g)
        add(*GROUPS[g])
    learn(len(GROUPS) - 1)
    pltpu.make_async_copy(last_ref, last_ref, recv_sem.at[len(GROUPS) - 1]).wait()
    sent = rows_ref.at[pl.ds(1, N_DEV - 1)]
    pltpu.make_async_copy(sent, sent, send_sem).wait()
    sent_ids = id_recv.at[pl.ds(1, N_DEV - 1)]
    pltpu.make_async_copy(sent_ids, sent_ids, id_send_sem).wait()


def finish(table_ref, last_ref, keys_ref, share_ref, table_hbm, share_hbm, stage, sems):
    share = pltpu.make_async_copy(share_ref, share_hbm, sems.at[len(PIECES)])
    share.start()
    n = GROUPS[-1][1]
    rows = last_ref[...].reshape(n * CAP, COLS)
    first = 0
    copies = [share]
    for i, size in enumerate(PIECES):
        at = lax.broadcasted_iota(jnp.int32, (size, 128), 0) + first
        keys = [keys_ref[LAST // 4 + j : LAST // 4 + j + 1, :] for j in range(n // 4)]
        hot = jnp.concatenate([(at == key).astype(jnp.bfloat16) for key in keys], axis=1)
        here = pl.ds(first, size)
        stage[here, :] = table_ref[here, :] + jnp.dot(hot, rows, preferred_element_type=jnp.float32)
        copy = pltpu.make_async_copy(stage.at[here], table_hbm.at[here], sems.at[i])
        copy.start()
        copies.append(copy)
        first += size
    for copy in copies:
        copy.wait()


def local(grads, token_ids):
    vmem = pl.BlockSpec(memory_space=pltpu.VMEM)
    hbm = pl.BlockSpec(memory_space=pltpu.HBM)
    dma = pltpu.SemaphoreType.DMA
    table, last, keys, share = pl.pallas_call(
        exchange,
        out_shape=(
            pltpu.VMEM((PAD_ROWS, COLS), jnp.float32),
            pltpu.VMEM((GROUPS[-1][1], CAP, COLS), jnp.bfloat16),
            pltpu.VMEM((CAP, 128), jnp.int32),
            pltpu.VMEM((HI_ROWS, 128), jnp.float32),
        ),
        in_specs=[hbm, hbm],
        out_specs=(vmem, vmem, vmem, vmem),
        scratch_shapes=[
            pltpu.VMEM((TOK_DEV, N_D * COLS), jnp.bfloat16),
            pltpu.VMEM((1, TOK_DEV), jnp.int32),
            pltpu.VMEM((N_D, N_V * CAP, COLS), jnp.bfloat16),
            pltpu.VMEM((N_V, 1, 128), jnp.int32),
            pltpu.VMEM((N_DEV, 1, 128), jnp.int32),
            pltpu.VMEM((N_DEV, CAP, COLS), jnp.bfloat16),
            dma, dma, dma, dma((len(GROUPS),)), dma, dma((len(GROUPS),)), dma,
            pltpu.SemaphoreType.REGULAR,
        ],
        compiler_params=pltpu.CompilerParams(collective_id=0, has_side_effects=True, vmem_limit_bytes=36 << 20),
        name="exchange",
    )(
        pltpu.with_memory_space_constraint(grads, pltpu.HBM),
        pltpu.with_memory_space_constraint(token_ids.reshape(1, TOK_DEV), pltpu.HBM),
    )
    table, share = pl.pallas_call(
        finish,
        out_shape=(
            jax.ShapeDtypeStruct((VOCAB_DEV, COLS), jnp.float32),
            jax.ShapeDtypeStruct((HI_ROWS, 128), jnp.float32),
        ),
        in_specs=[vmem, vmem, vmem, vmem],
        out_specs=(hbm, hbm),
        scratch_shapes=[pltpu.VMEM((VOCAB_DEV, COLS), jnp.float32), dma((len(PIECES) + 1,))],
        compiler_params=pltpu.CompilerParams(vmem_limit_bytes=32 << 20),
        name="finish",
    )(table, last, keys, share)
    return table, share.reshape(-1)[:VOCAB_DEV]


def solution(mesh):
    in_specs = (P(("vocab", "dp"), None), P(("vocab", "dp")))
    out_specs = (P("vocab", "dp"), P("vocab"))
    return jax.shard_map(local, mesh=mesh, in_specs=in_specs, out_specs=out_specs, check_vma=False)
```

```python
import jax
import jax.numpy as jnp
from jax import lax
from jax.experimental import pallas as pl
from jax.experimental.pallas import tpu as pltpu
from jax.sharding import PartitionSpec as P

VOCAB_DEV = 8016
TOK_DEV = 128
CAP = 32
COLS = 256
N_V = 8
N_D = 16
N_DEV = N_V * N_D
HI_ROWS = 64
PAD_ROWS = 8064
STRIPE = 4032
PIECES = (336, 1008) + (1344,) * 4 + (1296,)
MESH = pl.DeviceIdType.MESH
NT = (((1,), (1,)), ((), ()))

PLANE_A = [(i, 0, 0, j) for i in range(4) for j in range(2)]
PLANE_B = [(0, i, j, 0) for i in range(4) for j in range(4)]
NEAR = PLANE_A + PLANE_B[1:]
FAR = [
    (k // 2 % 4, (k // 2 + k // 8) % 4, (k // 2 + k // 8 + k // 32) % 4, k % 2)
    for k in range(N_DEV)
]
ORDER = NEAR + [o for o in FAR if o not in NEAR]
GROUPS = [(0, 16), (16, 16), (32, 16), (48, 16), (64, 16), (80, 16), (96, 16), (112, 16)]
AHEAD = 3
LAST = GROUPS[-1][0]


def exchange(grads_hbm, ids_hbm, table_ref, last_ref, keys_ref, share_ref, held, ids_ref, send, id_send, id_recv, rows_ref,
             load_sem, id_load_sem, send_sem, recv_sem, id_send_sem, id_recv_sem, own_sem, far_sem):
    v = lax.axis_index("vocab")
    d = lax.axis_index("dp")
    y, zl, zh, x, c = v // 2, v % 2, d // 8, (d // 2) % 4, d % 2
    z = 2 * zh + zl
    at_x = [2 * lax.rem(x + i, 4) for i in range(4)]
    at_y = [2 * lax.rem(y + i, 4) for i in range(4)]
    at_z = [lax.rem(z + i, 4) for i in range(4)]
    at_c = [c, 1 - c]
    vocab_at = [[at_y[i] + lax.rem(at_z[j], 2) for j in range(4)] for i in range(4)]
    data_at = [[at_x[i] + at_c[j] for j in range(2)] for i in range(4)]
    high_at = [8 * (at_z[j] // 2) for j in range(4)]

    def there(o):
        return vocab_at[o[1]][o[2]], data_at[o[0]][o[3]] + high_at[o[2]]

    barrier = pltpu.get_barrier_semaphore()
    for o in NEAR[1:]:
        pl.semaphore_signal(barrier, inc=1, device_id=there(o), device_id_type=MESH)
    id_load = pltpu.make_async_copy(ids_hbm, ids_ref, id_load_sem)
    id_load.start()
    load = pltpu.make_async_copy(grads_hbm, held, load_sem)
    load.start()

    id_load.wait()
    ids = ids_ref[...]
    owner = jnp.zeros_like(ids)
    for i in range(1, N_V):
        owner += (ids >= i * VOCAB_DEV).astype(jnp.int32)
    place = lax.broadcasted_iota(jnp.int32, (1, TOK_DEV), 1)
    for i in range(1, N_V):
        before = jnp.sum((owner < i).astype(jnp.int32), axis=1, keepdims=True)
        place = place - jnp.where(owner == i, before, 0)
    select = (lax.broadcasted_iota(jnp.int32, (N_V * CAP, TOK_DEV), 0) == owner * CAP + place).astype(jnp.bfloat16)
    inner = ids - owner * VOCAB_DEV
    mine = lax.broadcasted_iota(jnp.int32, (N_V, TOK_DEV), 0) == owner
    high = jnp.where(mine, inner // 128 + 1, 0).astype(jnp.bfloat16)
    low = jnp.where(mine, inner % 128, 0).astype(jnp.bfloat16)
    spread = (lax.broadcasted_iota(jnp.int32, (TOK_DEV, TOK_DEV), 0) % CAP == place).astype(jnp.bfloat16)
    high_of = lax.dot_general(high, spread, NT, preferred_element_type=jnp.float32)
    low_of = lax.dot_general(low, spread, NT, preferred_element_type=jnp.float32)
    slot_rows = ((high_of - 1.0) * 128.0 + low_of).astype(jnp.int32)
    for i in range(N_V):
        id_send[i] = slot_rows[i : i + 1, :]
    load.wait()
    for i in range(N_D):
        send[i] = jnp.dot(select, held[:, i * COLS : (i + 1) * COLS], preferred_element_type=jnp.float32).astype(jnp.bfloat16)

    def post(k):
        to_v, to_d = there(ORDER[k])
        group = next(g for g, (first, n) in enumerate(GROUPS) if first <= k < first + n)
        pltpu.make_async_remote_copy(
            id_send.at[to_v], id_recv.at[k], id_send_sem, id_recv_sem.at[group], device_id=(to_v, to_d), device_id_type=MESH
        ).start()
        pltpu.make_async_remote_copy(
            send.at[to_d, pl.ds(pl.multiple_of(to_v * CAP, CAP), CAP)],
            last_ref.at[k - LAST] if k >= LAST else rows_ref.at[k],
            send_sem, recv_sem.at[group], device_id=(to_v, to_d), device_id_type=MESH,
        ).start()

    pl.semaphore_wait(barrier, len(NEAR) - 1)
    for o in PLANE_B[1:]:
        pl.semaphore_signal(far_sem, inc=1, device_id=there(o), device_id_type=MESH)
    for k in range(1, len(NEAR)):
        post(k)
    own = pltpu.make_async_copy(send.at[d, pl.ds(pl.multiple_of(v * CAP, CAP), CAP)], rows_ref.at[0], own_sem)
    own.start()
    id_recv[0] = id_send[v]
    pl.semaphore_wait(far_sem, len(PLANE_B) - 1)
    for k in range(len(NEAR), sum(GROUPS[AHEAD - 1])):
        post(k)

    def post_after(g):
        if g + AHEAD < len(GROUPS):
            first, n = GROUPS[g + AHEAD]
            for k in range(first, first + n):
                post(k)

    quarter = lax.broadcasted_iota(jnp.int32, (1, 128), 1) // CAP
    tall = lax.broadcasted_iota(jnp.int32, (128, 128), 0)

    def learn(g):
        first, n = GROUPS[g]
        skip = int(g == 0)
        got = id_recv.at[pl.ds(first + skip, n - skip)]
        pltpu.make_async_copy(got, got, id_recv_sem.at[g]).wait()
        hot_high, hot_low = [], []
        for q in range(first // 4, (first + n) // 4):
            key = id_recv[4 * q]
            for i in range(1, 4):
                key = jnp.where(quarter == i, id_recv[4 * q + i], key)
            keys_ref[q : q + 1, :] = key
            hot_high.append((tall[:HI_ROWS] == key // 128).astype(jnp.bfloat16))
            hot_low.append((tall == key % 128).astype(jnp.bfloat16))
        found = lax.dot_general(
            jnp.concatenate(hot_high, axis=1), jnp.concatenate(hot_low, axis=1), NT, preferred_element_type=jnp.float32
        ) * (VOCAB_DEV / (TOK_DEV * N_D))
        if g == 0:
            share_ref[...] = found
        else:
            share_ref[...] += found

    def add(first, n, start=False):
        rows = rows_ref[pl.ds(first, n)].reshape(n * CAP, COLS)
        keys = [keys_ref[pl.ds(first // 4 + i, 1), :] for i in range(n // 4)]

        @pl.loop(0, PAD_ROWS // STRIPE)
        def _(t):
            at = lax.broadcasted_iota(jnp.int32, (STRIPE, 128), 0) + t * STRIPE
            hot = jnp.concatenate([(at == key).astype(jnp.bfloat16) for key in keys], axis=1)
            part = jnp.dot(hot, rows, preferred_element_type=jnp.float32)
            here = pl.ds(pl.multiple_of(t * STRIPE, STRIPE), STRIPE)
            if start:
                table_ref[here, :] = part
            else:
                table_ref[here, :] += part

    def arrived(first, n, group):
        got = rows_ref.at[pl.ds(first, n)]
        pltpu.make_async_copy(got, got, recv_sem.at[group]).wait()

    learn(0)
    own.wait()
    arrived(1, GROUPS[0][1] - 1, 0)
    post_after(0)
    add(0, GROUPS[0][1], True)
    for g in range(1, len(GROUPS) - 1):
        learn(g)
        arrived(*GROUPS[g], g)
        post_after(g)
        add(*GROUPS[g])
    learn(len(GROUPS) - 1)
    pltpu.make_async_copy(last_ref, last_ref, recv_sem.at[len(GROUPS) - 1]).wait()
    sent = rows_ref.at[pl.ds(1, N_DEV - 1)]
    pltpu.make_async_copy(sent, sent, send_sem).wait()
    sent_ids = id_recv.at[pl.ds(1, N_DEV - 1)]
    pltpu.make_async_copy(sent_ids, sent_ids, id_send_sem).wait()


def finish(table_ref, last_ref, keys_ref, share_ref, table_hbm, share_hbm, stage, sems):
    share = pltpu.make_async_copy(share_ref, share_hbm, sems.at[len(PIECES)])
    share.start()
    n = GROUPS[-1][1]
    rows = last_ref[...].reshape(n * CAP, COLS)
    first = 0
    copies = [share]
    for i, size in enumerate(PIECES):
        at = lax.broadcasted_iota(jnp.int32, (size, 128), 0) + first
        keys = [keys_ref[LAST // 4 + j : LAST // 4 + j + 1, :] for j in range(n // 4)]
        hot = jnp.concatenate([(at == key).astype(jnp.bfloat16) for key in keys], axis=1)
        here = pl.ds(first, size)
        stage[here, :] = table_ref[here, :] + jnp.dot(hot, rows, preferred_element_type=jnp.float32)
        copy = pltpu.make_async_copy(stage.at[here], table_hbm.at[here], sems.at[i])
        copy.start()
        copies.append(copy)
        first += size
    for copy in copies:
        copy.wait()


def local(grads, token_ids):
    vmem = pl.BlockSpec(memory_space=pltpu.VMEM)
    hbm = pl.BlockSpec(memory_space=pltpu.HBM)
    dma = pltpu.SemaphoreType.DMA
    table, last, keys, share = pl.pallas_call(
        exchange,
        out_shape=(
            pltpu.VMEM((PAD_ROWS, COLS), jnp.float32),
            pltpu.VMEM((GROUPS[-1][1], CAP, COLS), jnp.bfloat16),
            pltpu.VMEM((CAP, 128), jnp.int32),
            pltpu.VMEM((HI_ROWS, 128), jnp.float32),
        ),
        in_specs=[hbm, hbm],
        out_specs=(vmem, vmem, vmem, vmem),
        scratch_shapes=[
            pltpu.VMEM((TOK_DEV, N_D * COLS), jnp.bfloat16),
            pltpu.VMEM((1, TOK_DEV), jnp.int32),
            pltpu.VMEM((N_D, N_V * CAP, COLS), jnp.bfloat16),
            pltpu.VMEM((N_V, 1, 128), jnp.int32),
            pltpu.VMEM((N_DEV, 1, 128), jnp.int32),
            pltpu.VMEM((N_DEV, CAP, COLS), jnp.bfloat16),
            dma, dma, dma, dma((len(GROUPS),)), dma, dma((len(GROUPS),)), dma,
            pltpu.SemaphoreType.REGULAR,
        ],
        compiler_params=pltpu.CompilerParams(collective_id=0, has_side_effects=True, vmem_limit_bytes=36 << 20),
        name="exchange",
    )(
        pltpu.with_memory_space_constraint(grads, pltpu.HBM),
        pltpu.with_memory_space_constraint(token_ids.reshape(1, TOK_DEV), pltpu.HBM),
    )
    table, share = pl.pallas_call(
        finish,
        out_shape=(
            jax.ShapeDtypeStruct((VOCAB_DEV, COLS), jnp.float32),
            jax.ShapeDtypeStruct((HI_ROWS, 128), jnp.float32),
        ),
        in_specs=[vmem, vmem, vmem, vmem],
        out_specs=(hbm, hbm),
        scratch_shapes=[pltpu.VMEM((VOCAB_DEV, COLS), jnp.float32), dma((len(PIECES) + 1,))],
        compiler_params=pltpu.CompilerParams(vmem_limit_bytes=32 << 20),
        name="finish",
    )(table, last, keys, share)
    return table, share.reshape(-1)[:VOCAB_DEV]


def solution(mesh):
    in_specs = (P(("vocab", "dp"), None), P(("vocab", "dp")))
    out_specs = (P("vocab", "dp"), P("vocab"))
    return jax.shard_map(local, mesh=mesh, in_specs=in_specs, out_specs=out_specs, check_vma=False)
```
